128 devices in a mesh: rep: 2 (over core), dp: 64 (over x, y, z).
Axes of the slice: x: 4, y: 4, z: 4, core: 2. Of those that a mesh axis runs over, the one named last changes fastest.
Arguments:
- g_w_gate: bfloat16 [128, 2, 1024, 3200], P(('rep', 'dp')), parts along dimension 0
- g_w_up: bfloat16 [128, 2, 1024, 3200], P(('rep', 'dp')), parts along dimension 0
- g_w_down: bfloat16 [128, 2, 3200, 1024], P(('rep', 'dp')), parts along dimension 0
- w_gate: bfloat16 [2, 1024, 3200], replicated
- w_up: bfloat16 [2, 1024, 3200], replicated
- w_down: bfloat16 [2, 3200, 1024], replicated
- m_w_gate: float32 [2, 1024, 3200], P(None, 'dp')
- m_w_up: float32 [2, 1024, 3200], P(None, 'dp')
- m_w_down: float32 [2, 3200, 1024], P(None, 'dp')
- v_w_gate: float32 [2, 1024, 3200], P(None, 'dp')
- v_w_up: float32 [2, 1024, 3200], P(None, 'dp')
- v_w_down: float32 [2, 3200, 1024], P(None, 'dp')
Outputs:
- output 1: bfloat16 [4, 1024, 3200], P('rep'), parts along dimension 0
- output 2: bfloat16 [4, 1024, 3200], P('rep'), parts along dimension 0
- output 3: bfloat16 [4, 3200, 1024], P('rep'), parts along dimension 0
- output 4: float32 [4, 1024, 3200], P('rep', 'dp'), parts along dimension 0
- output 5: float32 [4, 1024, 3200], P('rep', 'dp'), parts along dimension 0
- output 6: float32 [4, 3200, 1024], P('rep', 'dp'), parts along dimension 0
- output 7: float32 [4, 1024, 3200], P('rep', 'dp'), parts along dimension 0
- output 8: float32 [4, 1024, 3200], P('rep', 'dp'), parts along dimension 0
- output 9: float32 [4, 3200, 1024], P('rep', 'dp'), parts along dimension 0
There are 2 independent parts. The reference program is written for one: setup_inputs(seed, part) draws one part's arguments, and reference() takes and returns one part's arrays. A program takes and returns all parts, laid end to end along the dimension named above; an argument that names none is the same for every part.
All inputs are finite; a program needn't handle non-finite values.
Results may differ from the reference program's by a relative error of at most 0.022.
Values are sent between devices in bfloat16 or wider.
A program may use at most 1.5 GiB of HBM per device.

```python
import jax
import jax.numpy as jnp
from jax import lax

DEVICES = 64
D = 1024
FF = 3200
LAYERS = 2
NAMES = ("w_gate", "w_up", "w_down")
SHAPES = {"w_gate": (LAYERS, D, FF), "w_up": (LAYERS, D, FF), "w_down": (LAYERS, FF, D)}


def setup_inputs(seed: int = 0, part: int = 0) -> dict:
    kz, *keys = jax.random.split(jax.random.key(seed), 1 + 5 * len(NAMES))
    loud = 2.0 ** jax.random.uniform(kz, (), jnp.float32, -1.0, 1.0)
    drawn = {}
    for name, key, both in zip(NAMES, keys[:3], keys[3:6], strict=True):
        own = jax.random.normal(jax.random.fold_in(key, part), (DEVICES, *SHAPES[name]), jnp.float32)
        shared = jax.random.normal(jax.random.fold_in(both, part), SHAPES[name], jnp.float32)
        drawn["g_" + name] = (loud * (0.7 * shared / DEVICES + 0.7 * own * DEVICES**-0.5)).astype(jnp.bfloat16)
    for name, key in zip(NAMES, keys[6:9], strict=True):
        drawn[name] = (jax.random.normal(key, SHAPES[name], jnp.float32) * SHAPES[name][1] ** -0.5).astype(jnp.bfloat16)
    for name, key in zip(NAMES, keys[9:12], strict=True):
        drawn["m_" + name] = loud * 0.5 * jax.random.normal(key, SHAPES[name], jnp.float32)
    for name, key in zip(NAMES, keys[12:15], strict=True):
        drawn["v_" + name] = loud * loud * jax.random.uniform(key, SHAPES[name], jnp.float32, 0.5, 1.5)
    return drawn


def adamw(w, m, v, g):
    m = 0.9 * m + 0.1 * g
    v = 0.95 * v + 0.05 * g * g
    step = m * lax.rsqrt(v + 1e-8) + 0.1 * w
    return (w - 0.02 * step).astype(jnp.bfloat16), m, v


def reference(g_w_gate, g_w_up, g_w_down, w_gate, w_up, w_down, m_w_gate, m_w_up, m_w_down, v_w_gate, v_w_up, v_w_down):
    def total(terms):
        return lax.scan(lambda so_far, term: (so_far + term.astype(jnp.float32), None), jnp.zeros(terms.shape[1:], jnp.float32), terms)[0]

    gradients = [total(terms).astype(jnp.bfloat16).astype(jnp.float32) for terms in (g_w_gate, g_w_up, g_w_down)]
    new = [
        adamw(w.astype(jnp.float32), m, v, g)
        for w, m, v, g in zip((w_gate, w_up, w_down), (m_w_gate, m_w_up, m_w_down), (v_w_gate, v_w_up, v_w_down), gradients, strict=True)
    ]
    return tuple(one[which] for which in range(3) for one in new)
```

```python
import functools

import jax
import jax.numpy as jnp
from jax import lax
from jax.experimental import pallas as pl
from jax.experimental.pallas import tpu as pltpu
from jax.sharding import PartitionSpec as P

F32, BF16 = jnp.float32, jnp.bfloat16
MESH = pl.DeviceIdType.MESH
STAGES = 12


class Part:
    def __init__(self, order, chunks, width, units, window, step, rows):
        self.order, self.chunks, self.width = order, chunks, width
        self.units, self.window, self.step, self.rows = units, window, step, rows
        self.down = window > 1


PARTS = (
    Part("yzx", 5, 640, 4, 1, 1, 16),
    Part("zxy", 5, 640, 4, 1, 1, 16),
    Part("xyz", 4, 256, 25, 7, 6, 8),
)
SCRATCH = ("G", "CB", "SA", "LA", "RA", "SB", "LB", "RB", "SC", "LC", "RC", "XC", "GO", "WN", "M", "mb", "vb", "wb", "send", "recv", "gsend", "grecv", "loc", "pre")


def scratch(p):
    k, u, w, r, n = p.chunks, p.units, p.width, p.rows, p.window
    slab = lambda *lead: pltpu.VMEM((*lead, 4, u, r, w), BF16)
    group = lambda *lead: pltpu.VMEM((*lead, u, r, w), BF16)
    win = lambda *lead: pltpu.VMEM((*lead, n, r, w), BF16)
    dma = pltpu.SemaphoreType.DMA
    return {
        "G": slab(k, 2), "CB": slab(2, 2), "SA": slab(k, 2), "LA": slab(k, 2), "RA": slab(k, 2),
        "SB": group(k, 2), "LB": group(k, 2), "RB": group(k, 2),
        "SC": win(k, 2), "LC": win(k, 2), "RC": win(k, 2), "XC": win(k, 4), "GO": win(k, 2),
        "WN": win(k, 4, 2) if p.down else win(k, 2),
        "M": group(k, 2) if p.down else pltpu.VMEM((8, 128), BF16),
        "mb": pltpu.VMEM((2, n, r, k * w), F32), "vb": pltpu.VMEM((2, n, r, k * w), F32), "wb": pltpu.VMEM((2, n, r, k * w), BF16),
        "send": dma((k, 3, 6)), "recv": dma((k, 3, 6)), "gsend": dma((k, 3, 4)), "grecv": dma((k, 3, 4)),
        "loc": dma((k, 5)), "pre": dma((3,)),
    }


class Later:
    def __init__(self, describe):
        self.describe = describe

    def start(self):
        self.describe().start()

    def wait(self):
        self.describe().wait()

    def wait_send(self):
        self.describe().wait_send()

    def wait_recv(self):
        self.describe().wait_recv()


class Run:
    def __init__(self, p, at, g, w, m, v, out, gout, **buffers):
        self.p, self.gh, self.wh, self.mh, self.vh, self.out, self.gout = p, g, w, m, v, out, gout
        self.at = at
        self.me = tuple(at[axis] for axis in p.order)
        self.__dict__.update(buffers)

    def device(self, phase, offset):
        to = dict(self.at)
        axis = self.p.order[phase]
        to[axis] = lax.rem(to[axis] + offset, 4)
        return {"dp": to["x"] * 16 + to["y"] * 4 + to["z"]}

    def near(self, phase, offset):
        return lax.rem(self.me[phase] + offset, 4)

    def cols(self, c):
        return pl.ds(pl.multiple_of(c * self.p.width, 128), self.p.width)

    def hbm(self, ref, layer, c, a=None, b=None, z=None):
        of = dict(zip(self.p.order, (a, b, z)))
        full = lambda axis: slice(None) if of[axis] is None else of[axis]
        if self.p.down:
            return ref.at[layer, full("x"), full("y"), :, :, self.cols(c)]
        return ref.at[layer, full("x"), full("y"), full("z"), :, self.cols(c)]

    def slab(self, ref, k, i, b):
        return ref.at[k, i, :, b] if self.p.order == "yzx" else ref.at[k, i, b]

    def unit(self, ref, k, i, b, j):
        return ref.at[k, i, j, b] if self.p.order == "yzx" else ref.at[k, i, b, j]

    def window(self, ref, k, i, z):
        return ref.at[k, i, pl.ds(z * self.p.step, self.p.window)]

    def to(self, src, dst, sems, phase, kind, c, offset):
        send, recv = sems
        return Later(
            lambda: pltpu.make_async_remote_copy(
                src_ref=src, dst_ref=dst, send_sem=send.at[c, phase, kind], recv_sem=recv.at[c, phase, kind],
                device_id=self.device(phase, offset), device_id_type=MESH,
            )
        )

    def rs(self, src, dst, phase, kind, c):
        return self.to(src, dst, (self.send, self.recv), phase, kind, c, 1 if kind % 2 == 0 else 3)

    def ag(self, src, dst, phase, kind, c):
        return self.to(src, dst, (self.gsend, self.grecv), phase, kind, c, 1 if kind % 2 == 0 else 3)

    def add(self, n, dst, *srcs):
        @pl.loop(0, n)
        def _(j):
            total = srcs[0](j)[...].astype(F32)
            for s in srcs[1:]:
                total = total + s(j)[...].astype(F32)
            dst(j)[...] = total.astype(BF16)

    def sum_copies(self, phase, c):
        rows = (self.SA, self.SB, self.SC)[phase], (self.LA, self.LB, self.LC)[phase], (self.RA, self.RB, self.RC)[phase]
        s, l, r = rows
        right, left, opposite = self.near(phase, 1), self.near(phase, 3), self.near(phase, 2)
        if phase == 0:
            src = [self.hbm(self.gh, i, c, a=a) for i, a in ((0, opposite), (1, opposite), (1, right), (0, left))]
        elif phase == 1:
            src = [self.slab(self.LA, c, i, b) for i, b in ((0, opposite), (1, opposite), (1, right), (0, left))]
        else:
            src = [self.XC.at[c, i] for i in range(4)]
        src += [s.at[c, 0], s.at[c, 1]]
        if phase == 0:
            src[4:] = [self.SA.at[c, 0], self.SA.at[c, 1]]
        dst = [s.at[c, 0], s.at[c, 1], l.at[c, 1], r.at[c, 0], l.at[c, 0], r.at[c, 1]]
        return [self.rs(src[kind], dst[kind], phase, kind, c) for kind in range(6)]

    def gather_place(self, phase, layer, c, offset):
        a, b, z = self.me
        if phase == 2:
            z = self.near(2, offset)
            return self.WN.at[c, z, layer] if self.p.down else self.hbm(self.out, layer, c, a, b, z)
        if phase == 1:
            return self.hbm(self.out, layer, c, a, self.near(1, offset))
        return self.hbm(self.out, layer, c, self.near(0, offset))

    def gather_copies(self, phase, c):
        both = pl.ds(0, 2)
        mine = self.gather_place(phase, both, c, 0)
        src = mine
        if phase == 2 and not self.p.down:
            src = self.WN.at[c, :, 0]
        if phase == 1 and self.p.down:
            src = self.M.at[c]
        first = self.gather_place(phase, 0, c, 3)
        second = self.gather_place(phase, 1, c, 1)
        return [
            self.ag(src, mine, phase, 0, c), self.ag(src, mine, phase, 1, c),
            self.ag(first, first, phase, 2, c), self.ag(second, second, phase, 3, c),
        ]

    def gather_arrivals(self, phase, c):
        both = pl.ds(0, 2)
        places = [(both, 3), (both, 1), (0, 2), (1, 2)]
        refs = [self.gather_place(phase, layer, c, offset) for layer, offset in places]
        return [self.ag(ref, ref, phase, kind, c) for kind, ref in enumerate(refs)]

    def local(self, c):
        a = self.me[0]
        b, z = self.me[1:]
        both = pl.ds(0, 2)
        copy = lambda *refs: Later(lambda: pltpu.make_async_copy(*refs))
        half = lax.rem(c, 2)
        if self.p.down:
            new = copy(self.M.at[c], self.hbm(self.out, both, c, a, b), self.loc.at[c, 3])
        else:
            new = copy(self.WN.at[c, :, 0], self.hbm(self.out, both, c, a, b, z), self.loc.at[c, 3])
        return [
            copy(self.hbm(self.gh, 0, c, a=self.near(0, 1)), self.CB.at[half, 0], self.loc.at[c, 0]),
            copy(self.hbm(self.gh, 1, c, a=self.near(0, 3)), self.CB.at[half, 1], self.loc.at[c, 1]),
            copy(self.hbm(self.gh, both, c, a=a), self.G.at[c], self.loc.at[c, 2]),
            new,
            copy(self.GO.at[c], self.gout.at[:, :, :, self.cols(c)], self.loc.at[c, 4]),
        ]

    def preload(self):
        a = self.at
        if self.p.down:
            w = self.wh.at[:, a["x"], a["y"], pl.ds(a["z"] * self.p.step, self.p.window)]
            dst = self.wb
        else:
            w, dst = self.wh.at[:, a["x"], a["y"], a["z"]], self.wb.at[:, 0]
        return [
            pltpu.make_async_copy(self.mh, self.mb, self.pre.at[0]),
            pltpu.make_async_copy(self.vh, self.vb, self.pre.at[1]),
            pltpu.make_async_copy(w, dst, self.pre.at[2]),
        ]

    def kept(self, c, i, b, j):
        return [lambda u, ref=ref: self.unit(ref, c, i, b, j(u)) for ref in (self.G, self.LA, self.RA)]

    def stage(self, s, c):
        p = self.p
        if s == 0:
            copies, local = self.sum_copies(0, c), self.local(c)
            for kind in (0, 1, 2, 3):
                copies[kind].start()
            for one in local[:3]:
                one.start()
        elif s == 1:
            copies, local = self.sum_copies(0, c), self.local(c)
            half = lax.rem(c, 2)
            for h in (0, 1):
                local[h].wait()
                copies[h].wait_recv()
                at = lambda ref, k: (lambda u: ref.at[k, h, lax.div(u, p.units), lax.rem(u, p.units)])
                self.add(4 * p.units, at(self.SA, c), at(self.SA, c), at(self.CB, half))
                copies[4 + h].start()
        elif s == 2:
            before, copies = self.sum_copies(0, c), self.sum_copies(1, c)
            for kind in (2, 3, 4, 5):
                before[kind].wait_recv()
            self.local(c)[2].wait()
            right, left, opposite = self.near(1, 1), self.near(1, 3), self.near(1, 2)
            for kind, (i, b) in enumerate(((0, opposite), (1, opposite), (1, right), (0, left))):
                srcs = self.kept(c, i, b, lambda u: u)
                self.add(p.units, srcs[1], *srcs)
                copies[kind].start()
        elif s == 3:
            copies = self.sum_copies(1, c)
            for h, b in ((0, self.near(1, 1)), (1, self.near(1, 3))):
                copies[h].wait_recv()
                dst = lambda u: self.SB.at[c, h, u]
                self.add(p.units, dst, *self.kept(c, h, b, lambda u: u), dst)
                copies[4 + h].start()
        elif s == 4:
            before, copies = self.sum_copies(1, c), self.sum_copies(2, c)
            for kind in (2, 3, 4, 5):
                before[kind].wait_recv()
            right, left, opposite = self.near(2, 1), self.near(2, 3), self.near(2, 2)
            for kind, (i, z) in enumerate(((0, opposite), (1, opposite), (1, right), (0, left))):
                self.add(p.window, lambda u: self.XC.at[c, kind, u], *self.own_sum(c, i, z))
                copies[kind].start()
        elif s == 5:
            copies = self.sum_copies(2, c)
            for h, z in ((0, self.near(2, 1)), (1, self.near(2, 3))):
                copies[h].wait_recv()
                dst = lambda u: self.SC.at[c, h, u]
                self.add(p.window, dst, *self.own_sum(c, h, z), dst)
                copies[4 + h].start()
        elif s == 6:
            before, copies, local = self.sum_copies(2, c), self.gather_copies(2, c), self.local(c)
            for kind in (2, 3, 4, 5):
                before[kind].wait_recv()

            @pl.when(c == 0)
            def _():
                for one in self.preload():
                    one.wait()

            self.update(c)
            copies[0].start()
            copies[1].start()
            local[4].start()
            if not p.down:
                local[3].start()
        elif s in (7, 9, 11):
            phase = {7: 2, 9: 1, 11: 0}[s]
            arrivals, copies = self.gather_arrivals(phase, c), self.gather_copies(phase, c)
            arrivals[0].wait_recv()
            copies[2].start()
            arrivals[1].wait_recv()
            copies[3].start()
        elif s == 8:
            arrivals, copies = self.gather_arrivals(2, c), self.gather_copies(1, c)
            arrivals[2].wait_recv()
            arrivals[3].wait_recv()
            if p.down:
                self.merge(c)
                self.local(c)[3].start()
            else:
                self.local(c)[3].wait()
            copies[0].start()
            copies[1].start()
        elif s == 10:
            arrivals, copies = self.gather_arrivals(1, c), self.gather_copies(0, c)
            arrivals[2].wait_recv()
            arrivals[3].wait_recv()
            if p.down:
                self.local(c)[3].wait()
            copies[0].start()
            copies[1].start()

    def own_sum(self, c, i, z):
        first = z * self.p.step
        place = lambda u: first + u
        srcs = self.kept(c, i, self.me[1], place)
        return [*srcs, *(lambda u, ref=ref: ref.at[c, i, place(u)] for ref in (self.LB, self.RB))]

    def update(self, c):
        p = self.p
        cols = self.cols(c)
        z = self.me[2]
        for i in (0, 1):
            srcs = [*self.own_sum(c, i, z), lambda u, i=i: self.LC.at[c, i, u], lambda u, i=i: self.RC.at[c, i, u]]

            @pl.loop(0, p.window)
            def _(u):
                total = srcs[0](u)[...].astype(F32)
                for s in srcs[1:]:
                    total = total + s(u)[...].astype(F32)
                g = total.astype(BF16)
                self.GO[c, i, u] = g
                g = g.astype(F32)
                m = 0.9 * self.mb[i, u, :, cols] + 0.1 * g
                v = 0.95 * self.vb[i, u, :, cols] + 0.05 * g * g
                w = self.wb[i, u, :, cols].astype(F32)
                w = (w - 0.02 * (m * lax.rsqrt(v + 1e-8) + 0.1 * w)).astype(BF16)
                if p.down:
                    self.WN[c, z, i, u] = w
                else:
                    self.WN[c, i, u] = w

    def merge(self, c):
        p = self.p
        row = lax.broadcasted_iota(jnp.int32, (p.rows, p.width), 0)
        for i in (0, 1):
            for z in range(4):
                low = 0 if z == 0 else 1
                high = 7 if z == 3 else 6

                @pl.loop(low, high)
                def _(u):
                    self.M[c, i, 6 * z + u] = self.WN[c, z, i, u]

                if z:
                    below = self.WN[c, z - 1, i, 6].astype(F32)
                    above = self.WN[c, z, i, 0].astype(F32)
                    self.M[c, i, 6 * z] = jnp.where(row < 2 * z, below, above).astype(BF16)

    def finish(self, c):
        for arrival in self.gather_arrivals(0, c)[2:]:
            arrival.wait_recv()
        for phase in range(3):
            for copy in (*self.sum_copies(phase, c), *self.gather_copies(phase, c)):
                copy.wait_send()
        self.local(c)[4].wait()


def kernel(*refs):
    ins, outs, rest = refs[:12], refs[12:18], refs[18:]
    i = lax.axis_index("dp")
    at = {"x": lax.div(i, 16), "y": lax.rem(lax.div(i, 4), 4), "z": lax.rem(i, 4)}
    runs = []
    for n, p in enumerate(PARTS):
        buffers = dict(zip(SCRATCH, rest[n * len(SCRATCH) : (n + 1) * len(SCRATCH)]))
        runs.append(Run(p, at, *(ins[n + 3 * which] for which in range(4)), outs[n], outs[n + 3], **buffers))
    last = max(p.chunks for p in PARTS) + STAGES - 1

    barrier = pltpu.get_barrier_semaphore()
    for phase in range(3):
        for offset in (1, 3):
            pl.semaphore_signal(barrier, inc=1, device_id=runs[0].device(phase, offset), device_id_type=MESH)
    pl.semaphore_wait(barrier, 6)
    for run in runs:
        for one in run.preload():
            one.start()

    @pl.loop(0, last)
    def _(t):
        for s in range(STAGES):
            for run in runs:

                @pl.when((t >= s) & (t - s < run.p.chunks))
                def _(run=run, s=s):
                    run.stage(s, t - s)

    for run in runs:

        @pl.loop(0, run.p.chunks)
        def _(c, run=run):
            run.finish(c)


def sum_step_gather(terms, weights, m, v):
    shapes = [(2, 4, 4, 4, 16, 3200)] * 2 + [(2, 4, 4, 25, 8, 1024)]
    own = [(2, 1, 16, 3200)] * 2 + [(2, 7, 8, 1024)]
    args = [a.reshape(s) for group, ss in ((terms, shapes), (weights, shapes), (m, own), (v, own)) for a, s in zip(group, ss, strict=True)]
    held = [one for p in PARTS for one in (lambda made: [made[name] for name in SCRATCH])(scratch(p))]
    hbm = pl.BlockSpec(memory_space=pl.ANY)
    return pl.pallas_call(
        kernel,
        name="sum_step_gather",
        out_shape=[jax.ShapeDtypeStruct(s, BF16) for s in (*shapes, *own)],
        in_specs=[hbm] * 12,
        out_specs=[hbm] * 6,
        scratch_shapes=held,
        compiler_params=pltpu.CompilerParams(collective_id=0, has_side_effects=True, vmem_limit_bytes=67_043_328),
    )(*args)


def solution(mesh):
    def step(*arrays):
        terms, weights, m, v = (arrays[i : i + 3] for i in (0, 3, 6, 9))
        z = lax.rem(lax.axis_index("dp"), 4)
        widen = lambda a: lax.dynamic_update_slice(jnp.zeros((2, 56, 1024), F32), a, (0, 2 * z, 0))
        out = sum_step_gather(terms, weights, [*m[:2], widen(m[2])], [*v[:2], widen(v[2])])
        new = [a.reshape(w.shape) for a, w in zip(out[:3], weights, strict=True)]
        g = [out[3].reshape(2, 16, 3200), out[4].reshape(2, 16, 3200)]
        g.append(lax.dynamic_slice(out[5].reshape(2, 56, 1024), (0, 2 * z, 0), (2, 50, 1024)))
        g = [a.astype(F32) for a in g]
        new_m = [0.9 * a + 0.1 * b for a, b in zip(m, g, strict=True)]
        new_v = [0.95 * a + 0.05 * b * b for a, b in zip(v, g, strict=True)]
        return (*new, *new_m, *new_v)

    all_of, cut = P(None, None, None), P(None, "dp", None)
    return jax.shard_map(
        step,
        mesh=mesh,
        in_specs=(P(("rep", "dp"), None, None, None),) * 3 + (all_of,) * 3 + (cut,) * 6,
        out_specs=(P("rep", None, None),) * 3 + (P("rep", "dp", None),) * 6,
        check_vma=False,
    )
```

```python
import functools

import jax
import jax.numpy as jnp
from jax import lax
from jax.experimental import pallas as pl
from jax.experimental.pallas import tpu as pltpu
from jax.sharding import PartitionSpec as P

F32, BF16 = jnp.float32, jnp.bfloat16
MESH = pl.DeviceIdType.MESH
STAGES = 12
VMEM_LIMIT = 24 << 20


class Part:
    def __init__(self, order, chunks, width, units, window, step, rows):
        self.order, self.chunks, self.width = order, chunks, width
        self.units, self.window, self.step, self.rows = units, window, step, rows
        self.down = window > 1


PARTS = (
    Part("yzx", 5, 640, 4, 1, 1, 16),
    Part("zxy", 5, 640, 4, 1, 1, 16),
    Part("xyz", 4, 256, 25, 7, 6, 8),
)
SCRATCH = ("CB", "SB", "LB", "RB", "SC", "LC", "RC", "XC", "WN", "mb", "vb", "wb", "send", "recv", "gsend", "grecv", "loc", "pre", "free")


def scratch(p):
    k, u, w, r, n = p.chunks, p.units, p.width, p.rows, p.window
    group = lambda *lead: pltpu.VMEM((*lead, u, r, w), BF16)
    win = lambda *lead: pltpu.VMEM((*lead, n, r, w), BF16)
    moment = pltpu.VMEM((2, n * r, k * w) if p.down else (8, 128), F32)
    dma = pltpu.SemaphoreType.DMA
    return {
        "CB": group(2, 2, 4), "SB": group(k, 2), "LB": group(k, 2), "RB": group(k, 2),
        "SC": win(k, 2), "LC": win(k, 2), "RC": win(k, 2), "XC": win(k, 4),
        "WN": win(k, 4, 2) if p.down else pltpu.VMEM((16, 128), BF16),
        "mb": moment, "vb": moment, "wb": pltpu.VMEM((2, n, r, k * w), BF16),
        "send": dma((k, 3, 6)), "recv": dma((k, 3, 6)), "gsend": dma((k, 3, 4)), "grecv": dma((k, 3, 4)),
        "loc": dma((k, 3)), "pre": dma((3,)), "free": pltpu.SemaphoreType.REGULAR((k, 3)),
    }


class Later:
    def __init__(self, describe):
        self.describe = describe

    def start(self):
        self.describe().start()

    def wait(self):
        self.describe().wait()

    def wait_send(self):
        self.describe().wait_send()

    def wait_recv(self):
        self.describe().wait_recv()


class Run:
    def __init__(self, p, at, g, w, m, v, out, mout, vout, **buffers):
        self.p, self.gh, self.wh, self.mh, self.vh = p, g, w, m, v
        self.out, self.mout, self.vout = out, mout, vout
        self.at = at
        self.me = tuple(at[axis] for axis in p.order)
        self.__dict__.update(buffers)

    def device(self, phase, offset):
        to = dict(self.at)
        axis = self.p.order[phase]
        to[axis] = lax.rem(to[axis] + offset, 4)
        return {"dp": to["x"] * 16 + to["y"] * 4 + to["z"]}

    def near(self, phase, offset):
        return lax.rem(self.me[phase] + offset, 4)

    def cols(self, c):
        return pl.ds(pl.multiple_of(c * self.p.width, 128), self.p.width)

    def part(self, ref, layer, c, a=None, b=None, z=None):
        of = dict(zip(self.p.order, (a, b, z)))
        full = lambda axis: slice(None) if of[axis] is None else of[axis]
        if self.p.down:
            units = slice(None) if z is None else z
            return ref.at[layer, full("x"), full("y"), units, :, self.cols(c)]
        return ref.at[layer, full("x"), full("y"), full("z"), :, self.cols(c)]

    def raw(self, i, q, first, second, c):
        where = {"yzx": (first, q, second), "zxy": (first, second, q), "xyz": (q, first, second)}[self.p.order]
        return self.out.at[(i, *where, slice(None), self.cols(c))]

    def to(self, src, dst, sems, phase, kind, c):
        send, recv = sems
        offset = 1 if kind % 2 == 0 else 3
        return Later(
            lambda: pltpu.make_async_remote_copy(
                src_ref=src, dst_ref=dst, send_sem=send.at[c, phase, kind], recv_sem=recv.at[c, phase, kind],
                device_id=self.device(phase, offset), device_id_type=MESH,
            )
        )

    def credit(self, phase, c):
        for offset in (1, 3):
            pl.semaphore_signal(self.free.at[c, phase], inc=1, device_id=self.device(phase, offset), device_id_type=MESH)

    def add(self, n, dst, *srcs):
        @pl.loop(0, n)
        def _(j):
            total = srcs[0](j)[...].astype(F32)
            for s in srcs[1:]:
                total = total + s(j)[...].astype(F32)
            dst(j)[...] = total.astype(BF16)

    def sum_copies(self, phase, c):
        right, left, opposite = self.near(phase, 1), self.near(phase, 3), self.near(phase, 2)
        kinds = ((0, opposite), (1, opposite), (1, right), (0, left))
        if phase == 0:
            mine = self.me[0]
            at = lambda i, a: self.part(self.out, i, c, a)
            src = [self.part(self.gh, i, c, a) for i, a in kinds] + [at(0, opposite), at(1, opposite)]
            dst = [at(0, left), at(1, right), at(1, mine), at(0, mine), at(0, mine), at(1, mine)]
        else:
            s, l, r = ((self.SB, self.LB, self.RB), (self.SC, self.LC, self.RC))[phase - 1]
            if phase == 1:
                src = [self.part(self.out, i, c, self.near(0, 3), b) for i, b in kinds]
            else:
                src = [self.XC.at[c, i] for i in range(4)]
            src += [s.at[c, 0], s.at[c, 1]]
            dst = [s.at[c, 0], s.at[c, 1], l.at[c, 1], r.at[c, 0], l.at[c, 0], r.at[c, 1]]
        return [self.to(src[kind], dst[kind], (self.send, self.recv), phase, kind, c) for kind in range(6)]

    def sum_arrivals(self, phase, c):
        if phase:
            return self.sum_copies(phase, c)
        right, left, opposite = self.near(0, 1), self.near(0, 3), self.near(0, 2)
        places = ((0, opposite), (1, opposite), (1, left), (0, right), (0, left), (1, right))
        refs = [self.part(self.out, i, c, a) for i, a in places]
        return [self.to(ref, ref, (self.send, self.recv), 0, kind, c) for kind, ref in enumerate(refs)]

    def gather_place(self, phase, layer, c, offset):
        a, b, z = self.me
        if phase == 2:
            z = self.near(2, offset)
            return self.WN.at[c, z, layer] if self.p.down else self.part(self.out, layer, c, a, b, z)
        if phase == 1:
            return self.part(self.out, layer, c, a, self.near(1, offset))
        return self.part(self.out, layer, c, self.near(0, offset))

    def gather_copies(self, phase, c):
        mine = self.gather_place(phase, pl.ds(0, 2), c, 0)
        first = self.gather_place(phase, 0, c, 3)
        second = self.gather_place(phase, 1, c, 1)
        sems = (self.gsend, self.grecv)
        return [self.to(ref, ref, sems, phase, kind, c) for kind, ref in enumerate((mine, mine, first, second))]

    def gather_arrivals(self, phase, c):
        both = pl.ds(0, 2)
        places = [(both, 3), (both, 1), (0, 2), (1, 2)]
        refs = [self.gather_place(phase, layer, c, offset) for layer, offset in places]
        return [self.to(ref, ref, (self.gsend, self.grecv), phase, kind, c) for kind, ref in enumerate(refs)]

    def local(self, c):
        copy = lambda *refs: Later(lambda: pltpu.make_async_copy(*refs))
        half, mine, both = lax.rem(c, 2), self.me[0], pl.ds(0, 2)
        return [
            copy(self.part(self.gh, 0, c, self.near(0, 1)), self.CB.at[half, 0], self.loc.at[c, 0]),
            copy(self.part(self.gh, 1, c, self.near(0, 3)), self.CB.at[half, 1], self.loc.at[c, 1]),
            copy(self.part(self.gh, both, c, mine), self.part(self.out, both, c, mine), self.loc.at[c, 2]),
        ]

    def preload(self):
        a = self.at
        if self.p.down:
            w = self.wh.at[:, a["x"], a["y"], pl.ds(a["z"] * self.p.step, self.p.window)]
            dst = self.wb
        else:
            w, dst = self.wh.at[:, a["x"], a["y"], a["z"]], self.wb.at[:, 0]
        return [
            pltpu.make_async_copy(self.mh, self.mout, self.pre.at[0]),
            pltpu.make_async_copy(self.vh, self.vout, self.pre.at[1]),
            pltpu.make_async_copy(w, dst, self.pre.at[2]),
        ]

    def kept(self, c, i, b, j):
        turned = self.p.order == "yzx"
        place = lambda u: (j(u), b) if turned else (b, j(u))
        return [lambda u, q=q: self.raw(i, q, *place(u), c) for q in (self.me[0], self.near(0, 3), self.near(0, 1))]

    def own_sum(self, c, i, z):
        first = z * self.p.step
        place = lambda u: first + u
        srcs = self.kept(c, i, self.me[1], place)
        return [*srcs, *(lambda u, ref=ref: ref.at[c, i, place(u)] for ref in (self.LB, self.RB))]

    def stage(self, s, c):
        p = self.p
        if s == 0:
            copies, local = self.sum_copies(0, c), self.local(c)
            for kind in (0, 1, 2, 3):
                copies[kind].start()
            for one in local:
                one.start()
        elif s == 1:
            arrivals, copies, local = self.sum_arrivals(0, c), self.sum_copies(0, c), self.local(c)
            half, opposite = lax.rem(c, 2), self.near(0, 2)
            for h in (0, 1):
                local[h].wait()
                arrivals[h].wait_recv()
                at = lambda u: (lax.div(u, p.units), lax.rem(u, p.units))
                dst = lambda u: self.raw(h, opposite, *at(u), c)
                self.add(4 * p.units, dst, dst, lambda u: self.CB.at[(half, h, *at(u))])
                copies[4 + h].start()
        elif s == 2:
            arrivals, copies = self.sum_arrivals(0, c), self.sum_copies(1, c)
            for kind in (2, 3, 4, 5):
                arrivals[kind].wait_recv()
            self.local(c)[2].wait()
            right, left, opposite = self.near(1, 1), self.near(1, 3), self.near(1, 2)
            for kind, (i, b) in enumerate(((0, opposite), (1, opposite), (1, right), (0, left))):
                srcs = self.kept(c, i, b, lambda u: u)
                self.add(p.units, srcs[1], *srcs)
                copies[kind].start()
        elif s == 3:
            copies = self.sum_copies(1, c)
            for h, b in ((0, self.near(1, 1)), (1, self.near(1, 3))):
                copies[h].wait_recv()
                dst = lambda u: self.SB.at[c, h, u]
                self.add(p.units, dst, *self.kept(c, h, b, lambda u: u), dst)
                copies[4 + h].start()
            self.credit(1, c)
        elif s == 4:
            before, copies = self.sum_copies(1, c), self.sum_copies(2, c)
            for kind in (2, 3, 4, 5):
                before[kind].wait_recv()
            right, left, opposite = self.near(2, 1), self.near(2, 3), self.near(2, 2)
            for kind, (i, z) in enumerate(((0, opposite), (1, opposite), (1, right), (0, left))):
                self.add(p.window, lambda u: self.XC.at[c, kind, u], *self.own_sum(c, i, z))
                copies[kind].start()
        elif s == 5:
            copies = self.sum_copies(2, c)
            for h, z in ((0, self.near(2, 1)), (1, self.near(2, 3))):
                copies[h].wait_recv()
                dst = lambda u: self.SC.at[c, h, u]
                self.add(p.window, dst, *self.own_sum(c, h, z), dst)
                copies[4 + h].start()
            if not p.down:
                self.credit(2, c)
        elif s == 6:
            before, copies = self.sum_copies(2, c), self.gather_copies(2, c)
            for kind in (2, 3, 4, 5):
                before[kind].wait_recv()

            @pl.when(c == 0)
            def _():
                for one in self.preload():
                    one.wait()
                if p.down:
                    self.moments(True)

            self.update(c)
            if not p.down:
                pl.semaphore_wait(self.free.at[c, 2], 2)
            copies[0].start()
            copies[1].start()
            for one in self.sent_from_out(c):
                one.wait_send()
            self.credit(0, c)
            if p.down:

                @pl.when(c == p.chunks - 1)
                def _():
                    self.moments(False)
        elif s in (7, 9, 11):
            phase = {7: 2, 9: 1, 11: 0}[s]
            arrivals, copies = self.gather_arrivals(phase, c), self.gather_copies(phase, c)
            arrivals[0].wait_recv()
            copies[2].start()
            arrivals[1].wait_recv()
            copies[3].start()
        elif s in (8, 10):
            phase = {8: 1, 10: 0}[s]
            arrivals, copies = self.gather_arrivals(phase + 1, c), self.gather_copies(phase, c)
            arrivals[2].wait_recv()
            arrivals[3].wait_recv()
            if s == 8 and p.down:
                self.merge(c)
            pl.semaphore_wait(self.free.at[c, phase], 2)
            copies[0].start()
            copies[1].start()

    def sent_from_out(self, c):
        return [*self.sum_copies(0, c)[4:], *self.sum_copies(1, c)[:4]]

    def update(self, c):
        p = self.p
        cols = self.cols(c)
        z = self.me[2]
        for i in (0, 1):
            srcs = [*self.own_sum(c, i, z), lambda u, i=i: self.LC.at[c, i, u], lambda u, i=i: self.RC.at[c, i, u]]

            @pl.loop(0, p.window)
            def _(u):
                total = srcs[0](u)[...].astype(F32)
                for s in srcs[1:]:
                    total = total + s(u)[...].astype(F32)
                g = total.astype(BF16).astype(F32)
                if p.down:
                    rows = pl.ds(pl.multiple_of(u * p.rows, p.rows), p.rows)
                    mr, vr = self.mb.at[i, rows, cols], self.vb.at[i, rows, cols]
                else:
                    mr, vr = self.mout.at[i, :, cols], self.vout.at[i, :, cols]
                m = 0.9 * mr[...] + 0.1 * g
                v = 0.95 * vr[...] + 0.05 * g * g
                w = self.wb[i, u, :, cols].astype(F32)
                w = (w - 0.02 * (m * lax.rsqrt(v + 1e-8) + 0.1 * w)).astype(BF16)
                mr[...] = m
                vr[...] = v
                if p.down:
                    self.WN[c, z, i, u] = w
                else:
                    self.part(self.out, i, c, *self.me)[...] = w

    def moments(self, into):
        first = 2 * self.at["z"]

        @pl.loop(0, 50)
        def _(r):
            for whole, held in ((self.mout, self.mb), (self.vout, self.vb)):
                for i in (0, 1):
                    if into:
                        held[i, pl.ds(first + r, 1), :] = whole[r, pl.ds(i, 1), :]
                    else:
                        whole[r, pl.ds(i, 1), :] = held[i, pl.ds(first + r, 1), :]

    def merge(self, c):
        p = self.p
        row = lax.broadcasted_iota(jnp.int32, (p.rows, p.width), 0)
        a, b = self.me[:2]
        for i in (0, 1):
            for z in range(4):
                low = 0 if z == 0 else 1
                high = 7 if z == 3 else 6

                @pl.loop(low, high)
                def _(u):
                    self.raw(i, a, b, 6 * z + u, c)[...] = self.WN[c, z, i, u]

                if z:
                    below = self.WN[c, z - 1, i, 6].astype(F32)
                    above = self.WN[c, z, i, 0].astype(F32)
                    self.raw(i, a, b, 6 * z, c)[...] = jnp.where(row < 2 * z, below, above).astype(BF16)

    def finish(self, c):
        for arrival in self.gather_arrivals(0, c)[2:]:
            arrival.wait_recv()
        waited = self.sum_copies(0, c)[:4] + self.sum_copies(1, c)[4:] + self.sum_copies(2, c)
        for phase in range(3):
            waited += self.gather_copies(phase, c)
        for copy in waited:
            copy.wait_send()


def kernel(*refs):
    ins, outs, rest = refs[:12], refs[12:21], refs[21:]
    i = lax.axis_index("dp")
    at = {"x": lax.div(i, 16), "y": lax.rem(lax.div(i, 4), 4), "z": lax.rem(i, 4)}
    runs = []
    for n, p in enumerate(PARTS):
        buffers = dict(zip(SCRATCH, rest[n * len(SCRATCH) : (n + 1) * len(SCRATCH)]))
        runs.append(Run(p, at, *ins[n::3], *outs[n::3], **buffers))
    last = max(p.chunks for p in PARTS) + STAGES - 1

    barrier = pltpu.get_barrier_semaphore()
    for phase in range(3):
        for offset in (1, 3):
            pl.semaphore_signal(barrier, inc=1, device_id=runs[0].device(phase, offset), device_id_type=MESH)
    pl.semaphore_wait(barrier, 6)
    for run in runs:
        for one in run.preload():
            one.start()

    @pl.loop(0, last)
    def _(t):
        for s in range(STAGES):
            for run in runs:

                @pl.when((t >= s) & (t - s < run.p.chunks))
                def _(run=run, s=s):
                    run.stage(s, t - s)

    for run in runs:

        @pl.loop(0, run.p.chunks)
        def _(c, run=run):
            run.finish(c)


def sum_step_gather(terms, weights, m, v):
    shapes = [(2, 4, 4, 4, 16, 3200)] * 2 + [(2, 4, 4, 25, 8, 1024)]
    moments = [a.shape for a in m]
    args = [a.reshape(s) for group in (terms, weights) for a, s in zip(group, shapes, strict=True)] + [*m, *v]
    held = [one for p in PARTS for one in (lambda made: [made[name] for name in SCRATCH])(scratch(p))]
    hbm = pl.BlockSpec(memory_space=pl.ANY)
    vmem = pl.BlockSpec(memory_space=pltpu.VMEM)
    made = pl.pallas_call(
        kernel,
        name="sum_step_gather",
        out_shape=[pltpu.VMEM(s, BF16) for s in shapes] + [pltpu.VMEM(s, F32) for s in moments * 2],
        in_specs=[hbm] * 12,
        out_specs=[vmem] * 9,
        scratch_shapes=held,
        compiler_params=pltpu.CompilerParams(collective_id=0, has_side_effects=True, vmem_limit_bytes=VMEM_LIMIT),
    )(*args)
    return pl.pallas_call(
        write_out,
        name="write_out",
        out_shape=[jax.ShapeDtypeStruct(a.shape, a.dtype) for a in made],
        in_specs=[vmem] * 9,
        out_specs=[hbm] * 9,
        scratch_shapes=[pltpu.SemaphoreType.DMA((9, 2))],
        compiler_params=pltpu.CompilerParams(vmem_limit_bytes=VMEM_LIMIT),
    )(*(pltpu.with_memory_space_constraint(a, pltpu.VMEM) for a in made))


def write_out(*refs):
    ins, outs, sems = refs[:9], refs[9:18], refs[18]
    copies = []
    for n, (src, dst) in enumerate(zip(ins, outs, strict=True)):
        if n < 3:
            copies += [pltpu.make_async_copy(src.at[i], dst.at[i], sems.at[n, i]) for i in (0, 1)]
        else:
            copies.append(pltpu.make_async_copy(src, dst, sems.at[n, 0]))
    for one in copies:
        one.start()
    for one in copies:
        one.wait()


def solution(mesh):
    def step(*arrays):
        terms, weights, m, v = (arrays[i : i + 3] for i in (0, 3, 6, 9))
        turn = lambda a: [*a[:2], a[2].transpose(1, 0, 2)]
        out = sum_step_gather(terms, weights, turn(m), turn(v))
        new = [a.reshape(w.shape) for a, w in zip(out[:3], weights, strict=True)]
        return (*new, *turn(out[3:6]), *turn(out[6:9]))

    all_of, cut = P(None, None, None), P(None, "dp", None)
    return jax.shard_map(
        step,
        mesh=mesh,
        in_specs=(P(("rep", "dp"), None, None, None),) * 3 + (all_of,) * 3 + (cut,) * 6,
        out_specs=(P("rep", None, None),) * 3 + (P("rep", "dp", None),) * 6,
        check_vma=False,
    )
```

```python
import functools

import jax
import jax.numpy as jnp
from jax import lax
from jax.experimental import pallas as pl
from jax.experimental.pallas import tpu as pltpu
from jax.sharding import PartitionSpec as P

F32, BF16 = jnp.float32, jnp.bfloat16
MESH = pl.DeviceIdType.MESH
STAGES = 12
GATE_CUTS = ((1, 1152), (2, 1024))
DOWN_CUTS = ((2, 384), (1, 256))
DOWN_BLOCK = 5
VMEM_LIMIT = 24 << 20


class Part:
    def __init__(self, order, cuts, units, window, step, rows, block):
        self.order, self.units, self.window, self.step, self.rows, self.block = order, units, window, step, rows, block
        self.down = window > 1
        self.chunks = sum(count for count, _ in cuts)
        self.widest = max(width for _, width in cuts)
        self.columns = sum(count * width for count, width in cuts)
        self.groups, chunk, column = [], 0, 0
        for count, width in cuts:
            self.groups.append((chunk, chunk + count, column, width))
            chunk, column = chunk + count, column + count * width


PARTS = (
    Part("yzx", GATE_CUTS, 4, 1, 1, 16, 4),
    Part("zxy", GATE_CUTS, 4, 1, 1, 16, 4),
    Part("xyz", DOWN_CUTS, 25, 7, 6, 8, DOWN_BLOCK),
)
SCRATCH = ("CB", "SB", "LB", "RB", "SC", "LC", "RC", "XC", "WN", "mb", "vb", "wb", "send", "recv", "gsend", "grecv", "loc", "pre", "free")


def scratch(p):
    k, u, w, r, n = p.chunks, p.units, p.widest, p.rows, p.window
    group = lambda *lead: pltpu.VMEM((*lead, u, r, w), BF16)
    win = lambda *lead: pltpu.VMEM((*lead, n, r, w), BF16)
    moment = pltpu.VMEM((2, n * r, p.columns) if p.down else (8, 128), F32)
    dma = pltpu.SemaphoreType.DMA
    return {
        "CB": group(2, 2, 4), "SB": group(k, 2, 2), "LB": group(k, 2), "RB": group(k, 2),
        "SC": win(k, 2, 2), "LC": win(k, 2), "RC": win(k, 2), "XC": win(k, 2),
        "WN": win(k, 4, 2) if p.down else pltpu.VMEM((16, 128), BF16),
        "mb": moment, "vb": moment, "wb": pltpu.VMEM((2, n, r, p.columns), BF16),
        "send": dma((k, 3, 6)), "recv": dma((k, 3, 6)), "gsend": dma((k, 3, 4)), "grecv": dma((k, 3, 4)),
        "loc": dma((k, 3)), "pre": dma((3,)), "free": pltpu.SemaphoreType.REGULAR((k, 3)),
    }


class Later:
    def __init__(self, describe):
        self.describe = describe

    def start(self):
        self.describe().start()

    def wait(self):
        self.describe().wait()

    def wait_send(self):
        self.describe().wait_send()

    def wait_recv(self):
        self.describe().wait_recv()


class Run:
    def __init__(self, p, at, g, w, m, v, out, mout, vout, **buffers):
        self.p, self.gh, self.wh, self.mh, self.vh = p, g, w, m, v
        self.out, self.mout, self.vout = out, mout, vout
        self.at = at
        self.me = tuple(at[axis] for axis in p.order)
        self.__dict__.update(buffers)

    def device(self, phase, offset):
        to = dict(self.at)
        axis = self.p.order[phase]
        to[axis] = lax.rem(to[axis] + offset, 4)
        return {"dp": to["x"] * 16 + to["y"] * 4 + to["z"]}

    def near(self, phase, offset):
        return lax.rem(self.me[phase] + offset, 4)

    def use(self, group):
        self.first, _, self.column, self.width = group
        return self

    def cols(self, c):
        return pl.ds(pl.multiple_of(self.column + (c - self.first) * self.width, 128), self.width)

    def cut(self, ref, *where):
        if self.width == self.p.widest:
            return ref.at[where]
        return ref.at[(*where, *[slice(None)] * (len(ref.shape) - len(where) - 1), pl.ds(0, self.width))]

    def part(self, ref, layer, c, a=None, b=None, z=None):
        of = dict(zip(self.p.order, (a, b, z)))
        full = lambda axis: slice(None) if of[axis] is None else of[axis]
        if self.p.down:
            units = slice(None) if z is None else z
            return ref.at[layer, full("x"), full("y"), units, :, self.cols(c)]
        return ref.at[layer, full("x"), full("y"), full("z"), :, self.cols(c)]

    def raw(self, i, q, first, second, c):
        where = {"yzx": (first, q, second), "zxy": (first, second, q), "xyz": (q, first, second)}[self.p.order]
        return self.out.at[(i, *where, slice(None), self.cols(c))]

    def to(self, src, dst, sems, phase, kind, c):
        send, recv = sems
        offset = 1 if kind % 2 == 0 else 3
        return Later(
            lambda: pltpu.make_async_remote_copy(
                src_ref=src, dst_ref=dst, send_sem=send.at[c, phase, kind], recv_sem=recv.at[c, phase, kind],
                device_id=self.device(phase, offset), device_id_type=MESH,
            )
        )

    def credit(self, phase, c):
        for offset in (1, 3):
            pl.semaphore_signal(self.free.at[c, phase], inc=1, device_id=self.device(phase, offset), device_id_type=MESH)

    def add(self, n, dst, *srcs):
        def one(j):
            total = srcs[0](j)[...].astype(F32)
            for s in srcs[1:]:
                total = total + s(j)[...].astype(F32)
            dst(j)[...] = total.astype(BF16)

        if n == 1:
            one(0)
        else:
            pl.loop(0, n)(one)

    def sum_copies(self, phase, c):
        right, left, opposite = self.near(phase, 1), self.near(phase, 3), self.near(phase, 2)
        kinds = ((0, opposite), (1, opposite), (1, right), (0, left))
        if phase == 0:
            mine = self.me[0]
            at = lambda i, a: self.part(self.out, i, c, a)
            src = [self.part(self.gh, i, c, a) for i, a in kinds] + [at(0, opposite), at(1, opposite)]
            dst = [at(0, left), at(1, right), at(1, mine), at(0, mine), at(0, mine), at(1, mine)]
        else:
            s, l, r = ((self.SB, self.LB, self.RB), (self.SC, self.LC, self.RC))[phase - 1]
            if phase == 1:
                src = [self.part(self.out, i, c, self.near(0, 3), opposite) for i in (0, 1)]
            else:
                src = [self.cut(self.XC, c, i) for i in (0, 1)]
            src += [self.cut(s, c, 0), self.cut(s, c, 1)]
            dst = [self.cut(s, c, 0, 0), self.cut(s, c, 1, 1), self.cut(l, c), self.cut(r, c)]
        return [self.to(one, there, (self.send, self.recv), phase, kind, c) for kind, (one, there) in enumerate(zip(src, dst, strict=True))]

    def sum_arrivals(self, phase, c):
        if phase:
            return self.sum_copies(phase, c)
        right, left, opposite = self.near(0, 1), self.near(0, 3), self.near(0, 2)
        places = ((0, opposite), (1, opposite), (1, left), (0, right), (0, left), (1, right))
        refs = [self.part(self.out, i, c, a) for i, a in places]
        return [self.to(ref, ref, (self.send, self.recv), 0, kind, c) for kind, ref in enumerate(refs)]

    def gather_place(self, phase, layer, c, offset):
        a, b, z = self.me
        if phase == 2:
            z = self.near(2, offset)
            return self.cut(self.WN, c, z, layer) if self.p.down else self.part(self.out, layer, c, a, b, z)
        if phase == 1:
            return self.part(self.out, layer, c, a, self.near(1, offset))
        return self.part(self.out, layer, c, self.near(0, offset))

    def gather_copies(self, phase, c):
        mine = self.gather_place(phase, pl.ds(0, 2), c, 0)
        first = self.gather_place(phase, 0, c, 3)
        second = self.gather_place(phase, 1, c, 1)
        sems = (self.gsend, self.grecv)
        return [self.to(ref, ref, sems, phase, kind, c) for kind, ref in enumerate((mine, mine, first, second))]

    def gather_arrivals(self, phase, c):
        both = pl.ds(0, 2)
        places = [(both, 3), (both, 1), (0, 2), (1, 2)]
        refs = [self.gather_place(phase, layer, c, offset) for layer, offset in places]
        return [self.to(ref, ref, (self.gsend, self.grecv), phase, kind, c) for kind, ref in enumerate(refs)]

    def local(self, c):
        copy = lambda *refs: Later(lambda: pltpu.make_async_copy(*refs))
        half, mine, both = lax.rem(c, 2), self.me[0], pl.ds(0, 2)
        return [
            copy(self.part(self.gh, 0, c, self.near(0, 1)), self.cut(self.CB, half, 0), self.loc.at[c, 0]),
            copy(self.part(self.gh, 1, c, self.near(0, 3)), self.cut(self.CB, half, 1), self.loc.at[c, 1]),
            copy(self.part(self.gh, both, c, mine), self.part(self.out, both, c, mine), self.loc.at[c, 2]),
        ]

    def preload(self):
        a = self.at
        if self.p.down:
            w = self.wh.at[:, a["x"], a["y"], pl.ds(a["z"] * self.p.step, self.p.window)]
            dst = self.wb
        else:
            w, dst = self.wh.at[:, a["x"], a["y"], a["z"]], self.wb.at[:, 0]
        return [
            pltpu.make_async_copy(self.mh, self.mout, self.pre.at[0]),
            pltpu.make_async_copy(self.vh, self.vout, self.pre.at[1]),
            pltpu.make_async_copy(w, dst, self.pre.at[2]),
        ]

    def kept(self, c, i, b, j):
        turned = self.p.order == "yzx"
        place = lambda u: (j(u), b) if turned else (b, j(u))
        return [lambda u, q=q: self.raw(i, q, *place(u), c) for q in (self.me[0], self.near(0, 3), self.near(0, 1))]

    def own_sum(self, c, i, z):
        place = lambda u: pl.ds(z * self.p.step, self.p.window)
        srcs = self.kept(c, i, self.me[1], place)
        return [*srcs, *(lambda u, ref=ref: self.cut(ref, c, i, place(u)) for ref in (self.LB, self.RB))]

    def stage(self, s, c):
        p = self.p
        block = lambda u: pl.ds(u * p.block, p.block)
        if s == 0:
            copies, local = self.sum_copies(0, c), self.local(c)
            for kind in (0, 1, 2, 3):
                copies[kind].start()
            for one in local:
                one.start()
        elif s == 1:
            arrivals, copies, local = self.sum_arrivals(0, c), self.sum_copies(0, c), self.local(c)
            half, opposite, blocks = lax.rem(c, 2), self.near(0, 2), p.units // p.block
            for h in (0, 1):
                local[h].wait()
                arrivals[h].wait_recv()
                at = lambda u: (lax.div(u, blocks), pl.ds(lax.rem(u, blocks) * p.block, p.block))
                dst = lambda u: self.raw(h, opposite, *at(u), c)
                self.add(4 * blocks, dst, dst, lambda u: self.cut(self.CB, half, h, *at(u)))
                copies[4 + h].start()
        elif s == 2:
            arrivals, copies = self.sum_arrivals(0, c), self.sum_copies(1, c)
            for kind in (2, 3, 4, 5):
                arrivals[kind].wait_recv()
            self.local(c)[2].wait()
            right, left, opposite = self.near(1, 1), self.near(1, 3), self.near(1, 2)
            blocks = p.units // p.block
            for i in (0, 1):
                srcs = self.kept(c, i, opposite, block)
                self.add(blocks, srcs[1], *srcs)
                copies[i].start()
            for way, i, b in ((0, 1, right), (1, 0, left)):
                self.add(blocks, lambda u: self.cut(self.SB, c, way, i, block(u)), *self.kept(c, i, b, block))
        elif s == 3:
            copies = self.sum_copies(1, c)
            for h, b in ((0, self.near(1, 1)), (1, self.near(1, 3))):
                copies[h].wait_recv()
                dst = lambda u: self.cut(self.SB, c, h, h, block(u))
                self.add(p.units // p.block, dst, *self.kept(c, h, b, block), dst)
                copies[2 + h].start()
            self.credit(1, c)
        elif s == 4:
            before, copies = self.sum_copies(1, c), self.sum_copies(2, c)
            for kind in (2, 3):
                before[kind].wait_recv()
            right, left, opposite = self.near(2, 1), self.near(2, 3), self.near(2, 2)
            for i in (0, 1):
                self.add(1, lambda u: self.cut(self.XC, c, i), *self.own_sum(c, i, opposite))
                copies[i].start()
            for way, i, z in ((0, 1, right), (1, 0, left)):
                self.add(1, lambda u: self.cut(self.SC, c, way, i), *self.own_sum(c, i, z))
        elif s == 5:
            copies = self.sum_copies(2, c)
            for h, z in ((0, self.near(2, 1)), (1, self.near(2, 3))):
                copies[h].wait_recv()
                dst = lambda u: self.cut(self.SC, c, h, h)
                self.add(1, dst, *self.own_sum(c, h, z), dst)
                copies[2 + h].start()
            if not p.down:
                self.credit(2, c)
        elif s == 6:
            before, copies = self.sum_copies(2, c), self.gather_copies(2, c)
            for kind in (2, 3):
                before[kind].wait_recv()

            @pl.when(c == 0)
            def _():
                for one in self.preload():
                    one.wait()
                if p.down:
                    self.moments(True)

            self.update(c)
            if not p.down:
                pl.semaphore_wait(self.free.at[c, 2], 2)
            copies[0].start()
            copies[1].start()
            for one in self.sent_from_out(c):
                one.wait_send()
            self.credit(0, c)
            if p.down:

                @pl.when(c == p.chunks - 1)
                def _():
                    self.moments(False)
        elif s in (7, 9, 11):
            phase = {7: 2, 9: 1, 11: 0}[s]
            arrivals, copies = self.gather_arrivals(phase, c), self.gather_copies(phase, c)
            arrivals[0].wait_recv()
            copies[2].start()
            arrivals[1].wait_recv()
            copies[3].start()
        elif s in (8, 10):
            phase = {8: 1, 10: 0}[s]
            arrivals, copies = self.gather_arrivals(phase + 1, c), self.gather_copies(phase, c)
            arrivals[2].wait_recv()
            arrivals[3].wait_recv()
            if s == 8 and p.down:
                self.merge(c)
            pl.semaphore_wait(self.free.at[c, phase], 2)
            copies[0].start()
            copies[1].start()

    def sent_from_out(self, c):
        return [*self.sum_copies(0, c)[4:], *self.sum_copies(1, c)[:2]]

    def update(self, c):
        p = self.p
        cols = self.cols(c)
        z = self.me[2]
        for i in (0, 1):
            srcs = [*self.own_sum(c, i, z), *(lambda u, ref=ref: self.cut(ref, c, i) for ref in (self.LC, self.RC))]
            total = srcs[0](0)[...].astype(F32)
            for s in srcs[1:]:
                total = total + s(0)[...].astype(F32)
            g = total.astype(BF16).astype(F32).reshape(p.window * p.rows, self.width)
            mr, vr = (self.mb, self.vb) if p.down else (self.mout, self.vout)
            m = 0.9 * mr[i, :, cols] + 0.1 * g
            v = 0.95 * vr[i, :, cols] + 0.05 * g * g
            w = self.wb[i, :, :, cols].astype(F32).reshape(p.window * p.rows, self.width)
            w = (w - 0.02 * (m * lax.rsqrt(v + 1e-8) + 0.1 * w)).reshape(p.window, p.rows, self.width).astype(BF16)
            mr[i, :, cols] = m
            vr[i, :, cols] = v
            if p.down:
                self.cut(self.WN, c, z, i)[...] = w
            else:
                self.part(self.out, i, c, *self.me)[...] = w[0]

    def moments(self, into):
        first = 2 * self.at["z"]

        @pl.loop(0, 50)
        def _(r):
            for whole, held in ((self.mout, self.mb), (self.vout, self.vb)):
                for i in (0, 1):
                    if into:
                        held[i, pl.ds(first + r, 1), :] = whole[r, pl.ds(i, 1), :]
                    else:
                        whole[r, pl.ds(i, 1), :] = held[i, pl.ds(first + r, 1), :]

    def merge(self, c):
        p = self.p
        row = lax.broadcasted_iota(jnp.int32, (p.rows, self.width), 0)
        a, b = self.me[:2]
        for i in (0, 1):
            for z in range(4):
                low = 0 if z == 0 else 1
                high = 7 if z == 3 else 6
                self.raw(i, a, b, pl.ds(6 * z + low, high - low), c)[...] = self.cut(self.WN, c, z, i, pl.ds(low, high - low))[...]
                if z:
                    below = self.cut(self.WN, c, z - 1, i, 6)[...].astype(F32)
                    above = self.cut(self.WN, c, z, i, 0)[...].astype(F32)
                    self.raw(i, a, b, 6 * z, c)[...] = jnp.where(row < 2 * z, below, above).astype(BF16)

    def finish(self, c):
        for arrival in self.gather_arrivals(0, c)[2:]:
            arrival.wait_recv()
        waited = self.sum_copies(0, c)[:4] + self.sum_copies(1, c)[2:] + self.sum_copies(2, c)
        for phase in range(3):
            waited += self.gather_copies(phase, c)
        for copy in waited:
            copy.wait_send()


def kernel(*refs):
    ins, outs, rest = refs[:12], refs[12:21], refs[21:]
    i = lax.axis_index("dp")
    at = {"x": lax.div(i, 16), "y": lax.rem(lax.div(i, 4), 4), "z": lax.rem(i, 4)}
    runs = []
    for n, p in enumerate(PARTS):
        buffers = dict(zip(SCRATCH, rest[n * len(SCRATCH) : (n + 1) * len(SCRATCH)]))
        runs.append(Run(p, at, *ins[n::3], *outs[n::3], **buffers))
    last = max(p.chunks for p in PARTS) + STAGES - 1

    barrier = pltpu.get_barrier_semaphore()
    for phase in range(3):
        for offset in (1, 3):
            pl.semaphore_signal(barrier, inc=1, device_id=runs[0].device(phase, offset), device_id_type=MESH)
    pl.semaphore_wait(barrier, 6)
    for run in runs:
        for one in run.preload():
            one.start()

    @pl.loop(0, last)
    def _(t):
        for s in range(STAGES):
            for run in runs:
                for group in run.p.groups:

                    @pl.when((t - s >= group[0]) & (t - s < group[1]))
                    def _(run=run, s=s, group=group):
                        run.use(group).stage(s, t - s)

    for run in runs:
        for group in run.p.groups:

            @pl.loop(group[0], group[1])
            def _(c, run=run, group=group):
                run.use(group).finish(c)


def sum_step_gather(terms, weights, m, v):
    shapes = [(2, 4, 4, 4, 16, 3200)] * 2 + [(2, 4, 4, 25, 8, 1024)]
    moments = [a.shape for a in m]
    args = [a.reshape(s) for group in (terms, weights) for a, s in zip(group, shapes, strict=True)] + [*m, *v]
    held = [one for p in PARTS for one in (lambda made: [made[name] for name in SCRATCH])(scratch(p))]
    hbm = pl.BlockSpec(memory_space=pl.ANY)
    vmem = pl.BlockSpec(memory_space=pltpu.VMEM)
    made = pl.pallas_call(
        kernel,
        name="sum_step_gather",
        out_shape=[pltpu.VMEM(s, BF16) for s in shapes] + [pltpu.VMEM(s, F32) for s in moments * 2],
        in_specs=[hbm] * 12,
        out_specs=[vmem] * 9,
        scratch_shapes=held,
        compiler_params=pltpu.CompilerParams(collective_id=0, has_side_effects=True, vmem_limit_bytes=VMEM_LIMIT),
    )(*args)
    return pl.pallas_call(
        write_out,
        name="write_out",
        out_shape=[jax.ShapeDtypeStruct(a.shape, a.dtype) for a in made],
        in_specs=[vmem] * 9,
        out_specs=[hbm] * 9,
        scratch_shapes=[pltpu.SemaphoreType.DMA((9, 2))],
        compiler_params=pltpu.CompilerParams(vmem_limit_bytes=VMEM_LIMIT),
    )(*(pltpu.with_memory_space_constraint(a, pltpu.VMEM) for a in made))


def write_out(*refs):
    ins, outs, sems = refs[:9], refs[9:18], refs[18]
    copies = []
    for n, (src, dst) in enumerate(zip(ins, outs, strict=True)):
        if n < 3:
            copies += [pltpu.make_async_copy(src.at[i], dst.at[i], sems.at[n, i]) for i in (0, 1)]
        else:
            copies.append(pltpu.make_async_copy(src, dst, sems.at[n, 0]))
    for one in copies:
        one.start()
    for one in copies:
        one.wait()


def solution(mesh):
    def step(*arrays):
        terms, weights, m, v = (arrays[i : i + 3] for i in (0, 3, 6, 9))
        turn = lambda a: [*a[:2], a[2].transpose(1, 0, 2)]
        out = sum_step_gather(terms, weights, turn(m), turn(v))
        new = [a.reshape(w.shape) for a, w in zip(out[:3], weights, strict=True)]
        return (*new, *turn(out[3:6]), *turn(out[6:9]))

    all_of, cut = P(None, None, None), P(None, "dp", None)
    return jax.shard_map(
        step,
        mesh=mesh,
        in_specs=(P(("rep", "dp"), None, None, None),) * 3 + (all_of,) * 3 + (cut,) * 6,
        out_specs=(P("rep", None, None),) * 3 + (P("rep", "dp", None),) * 6,
        check_vma=False,
    )
```

```python
import functools

import jax
import jax.numpy as jnp
from jax import lax
from jax.experimental import pallas as pl
from jax.experimental.pallas import tpu as pltpu
from jax.sharding import PartitionSpec as P

F32, BF16 = jnp.float32, jnp.bfloat16
MESH = pl.DeviceIdType.MESH
STAGES = 12
GATE_CUTS = ((1, 1152), (2, 1024))
DOWN_CUTS = ((2, 384), (1, 256))
DOWN_BLOCK = 5
VMEM_LIMIT = 24 << 20


class Part:
    def __init__(self, order, cuts, units, window, step, rows, block):
        self.order, self.units, self.window, self.step, self.rows, self.block = order, units, window, step, rows, block
        self.down = window > 1
        self.chunks = sum(count for count, _ in cuts)
        self.widest = max(width for _, width in cuts)
        self.columns = sum(count * width for count, width in cuts)
        self.groups, chunk, column = [], 0, 0
        for count, width in cuts:
            self.groups.append((chunk, chunk + count, column, width))
            chunk, column = chunk + count, column + count * width


PARTS = (
    Part("yzx", GATE_CUTS, 4, 1, 1, 16, 4),
    Part("zxy", GATE_CUTS, 4, 1, 1, 16, 4),
    Part("xyz", DOWN_CUTS, 25, 7, 6, 8, DOWN_BLOCK),
)
SCRATCH = ("CB", "SB", "LB", "RB", "SC", "LC", "RC", "XC", "WN", "mb", "vb", "wb", "send", "recv", "gsend", "grecv", "loc", "pre", "free")


def scratch(p):
    k, u, w, r, n = p.chunks, p.units, p.widest, p.rows, p.window
    group = lambda *lead: pltpu.VMEM((*lead, u, r, w), BF16)
    win = lambda *lead: pltpu.VMEM((*lead, n, r, w), BF16)
    moment = pltpu.VMEM((2, n * r, p.columns) if p.down else (8, 128), F32)
    dma = pltpu.SemaphoreType.DMA
    return {
        "CB": group(2, 2, 4), "SB": group(k, 2, 2), "LB": group(k, 2), "RB": group(k, 2),
        "SC": win(k, 2, 2), "LC": win(k, 2), "RC": win(k, 2), "XC": win(k, 2),
        "WN": win(k, 4, 2) if p.down else pltpu.VMEM((16, 128), BF16),
        "mb": moment, "vb": moment, "wb": pltpu.VMEM((2, n, r, p.columns), BF16),
        "send": dma((k, 3, 6)), "recv": dma((k, 3, 6)), "gsend": dma((k, 3, 4)), "grecv": dma((k, 3, 4)),
        "loc": dma((k, 3)), "pre": dma((3,)), "free": pltpu.SemaphoreType.REGULAR((k, 3)),
    }


class Later:
    def __init__(self, describe):
        self.describe = describe

    def start(self):
        self.describe().start()

    def wait(self):
        self.describe().wait()

    def wait_send(self):
        self.describe().wait_send()

    def wait_recv(self):
        self.describe().wait_recv()


class Run:
    def __init__(self, p, at, g, w, m, v, out, mout, vout, **buffers):
        self.p, self.gh, self.wh, self.mh, self.vh = p, g, w, m, v
        self.out, self.mout, self.vout = out, mout, vout
        self.at = at
        self.me = tuple(at[axis] for axis in p.order)
        self.__dict__.update(buffers)

    def device(self, phase, offset):
        to = dict(self.at)
        axis = self.p.order[phase]
        to[axis] = lax.rem(to[axis] + offset, 4)
        return {"dp": to["x"] * 16 + to["y"] * 4 + to["z"]}

    def near(self, phase, offset):
        return lax.rem(self.me[phase] + offset, 4)

    def use(self, group):
        self.first, _, self.column, self.width = group
        return self

    def cols(self, c):
        return pl.ds(pl.multiple_of(self.column + (c - self.first) * self.width, 128), self.width)

    def cut(self, ref, *where):
        if self.width == self.p.widest:
            return ref.at[where]
        return ref.at[(*where, *[slice(None)] * (len(ref.shape) - len(where) - 1), pl.ds(0, self.width))]

    def part(self, ref, layer, c, a=None, b=None, z=None):
        of = dict(zip(self.p.order, (a, b, z)))
        full = lambda axis: slice(None) if of[axis] is None else of[axis]
        if self.p.down:
            units = slice(None) if z is None else z
            return ref.at[layer, full("x"), full("y"), units, :, self.cols(c)]
        return ref.at[layer, full("x"), full("y"), full("z"), :, self.cols(c)]

    def raw(self, i, q, first, second, c):
        where = {"yzx": (first, q, second), "zxy": (first, second, q), "xyz": (q, first, second)}[self.p.order]
        return self.out.at[(i, *where, slice(None), self.cols(c))]

    def to(self, src, dst, sems, phase, kind, c):
        send, recv = sems
        offset = 1 if kind % 2 == 0 else 3
        return Later(
            lambda: pltpu.make_async_remote_copy(
                src_ref=src, dst_ref=dst, send_sem=send.at[c, phase, kind], recv_sem=recv.at[c, phase, kind],
                device_id=self.device(phase, offset), device_id_type=MESH,
            )
        )

    def credit(self, phase, c):
        for offset in (1, 3):
            pl.semaphore_signal(self.free.at[c, phase], inc=1, device_id=self.device(phase, offset), device_id_type=MESH)

    def add(self, n, dst, *srcs):
        def one(j):
            total = srcs[0](j)[...].astype(F32)
            for s in srcs[1:]:
                total = total + s(j)[...].astype(F32)
            dst(j)[...] = total.astype(BF16)

        if n == 1:
            one(0)
        else:
            pl.loop(0, n)(one)

    def sum_copies(self, phase, c):
        right, left, opposite = self.near(phase, 1), self.near(phase, 3), self.near(phase, 2)
        kinds = ((0, opposite), (1, opposite), (1, right), (0, left))
        if phase == 0:
            mine = self.me[0]
            at = lambda i, a: self.part(self.out, i, c, a)
            src = [self.part(self.gh, i, c, a) for i, a in kinds] + [at(0, opposite), at(1, opposite)]
            dst = [at(0, left), at(1, right), at(1, mine), at(0, mine), at(0, mine), at(1, mine)]
        else:
            s, l, r = ((self.SB, self.LB, self.RB), (self.SC, self.LC, self.RC))[phase - 1]
            if phase == 1:
                src = [self.part(self.out, i, c, self.near(0, 3), opposite) for i in (0, 1)]
            else:
                src = [self.cut(self.XC, c, i) for i in (0, 1)]
            src += [self.cut(s, c, 0), self.cut(s, c, 1)]
            dst = [self.cut(s, c, 0, 0), self.cut(s, c, 1, 1), self.cut(l, c), self.cut(r, c)]
        return [self.to(one, there, (self.send, self.recv), phase, kind, c) for kind, (one, there) in enumerate(zip(src, dst, strict=True))]

    def sum_arrivals(self, phase, c):
        if phase:
            return self.sum_copies(phase, c)
        right, left, opposite = self.near(0, 1), self.near(0, 3), self.near(0, 2)
        places = ((0, opposite), (1, opposite), (1, left), (0, right), (0, left), (1, right))
        refs = [self.part(self.out, i, c, a) for i, a in places]
        return [self.to(ref, ref, (self.send, self.recv), 0, kind, c) for kind, ref in enumerate(refs)]

    def gather_place(self, phase, layer, c, offset):
        a, b, z = self.me
        if phase == 2:
            z = self.near(2, offset)
            return self.cut(self.WN, c, z, layer) if self.p.down else self.part(self.out, layer, c, a, b, z)
        if phase == 1:
            return self.part(self.out, layer, c, a, self.near(1, offset))
        return self.part(self.out, layer, c, self.near(0, offset))

    def gather_copies(self, phase, c):
        mine = self.gather_place(phase, pl.ds(0, 2), c, 0)
        first = self.gather_place(phase, 0, c, 3)
        second = self.gather_place(phase, 1, c, 1)
        sems = (self.gsend, self.grecv)
        return [self.to(ref, ref, sems, phase, kind, c) for kind, ref in enumerate((mine, mine, first, second))]

    def gather_arrivals(self, phase, c):
        both = pl.ds(0, 2)
        places = [(both, 3), (both, 1), (0, 2), (1, 2)]
        refs = [self.gather_place(phase, layer, c, offset) for layer, offset in places]
        return [self.to(ref, ref, (self.gsend, self.grecv), phase, kind, c) for kind, ref in enumerate(refs)]

    def local(self, c):
        copy = lambda *refs: Later(lambda: pltpu.make_async_copy(*refs))
        half, mine, both = lax.rem(c, 2), self.me[0], pl.ds(0, 2)
        return [
            copy(self.part(self.gh, 0, c, self.near(0, 1)), self.cut(self.CB, half, 0), self.loc.at[c, 0]),
            copy(self.part(self.gh, 1, c, self.near(0, 3)), self.cut(self.CB, half, 1), self.loc.at[c, 1]),
            copy(self.part(self.gh, both, c, mine), self.part(self.out, both, c, mine), self.loc.at[c, 2]),
        ]

    def preload(self):
        a = self.at
        if self.p.down:
            w = self.wh.at[:, a["x"], a["y"], pl.ds(a["z"] * self.p.step, self.p.window)]
            dst = self.wb
        else:
            w, dst = self.wh.at[:, a["x"], a["y"], a["z"]], self.wb.at[:, 0]
        return [
            pltpu.make_async_copy(self.mh, self.mout, self.pre.at[0]),
            pltpu.make_async_copy(self.vh, self.vout, self.pre.at[1]),
            pltpu.make_async_copy(w, dst, self.pre.at[2]),
        ]

    def kept(self, c, i, b, j):
        turned = self.p.order == "yzx"
        place = lambda u: (j(u), b) if turned else (b, j(u))
        return [lambda u, q=q: self.raw(i, q, *place(u), c) for q in (self.me[0], self.near(0, 3), self.near(0, 1))]

    def own_sum(self, c, i, z):
        place = lambda u: pl.ds(z * self.p.step, self.p.window)
        srcs = self.kept(c, i, self.me[1], place)
        return [*srcs, *(lambda u, ref=ref: self.cut(ref, c, i, place(u)) for ref in (self.LB, self.RB))]

    def stage(self, s, c):
        p = self.p
        block = lambda u: pl.ds(u * p.block, p.block)
        if s == 0:
            copies, local = self.sum_copies(0, c), self.local(c)
            for kind in (0, 1, 2, 3):
                copies[kind].start()
            for one in local:
                one.start()
        elif s == 1:
            arrivals, copies, local = self.sum_arrivals(0, c), self.sum_copies(0, c), self.local(c)
            half, opposite, blocks = lax.rem(c, 2), self.near(0, 2), p.units // p.block
            for h in (0, 1):
                local[h].wait()
                arrivals[h].wait_recv()
                at = lambda u: (lax.div(u, blocks), pl.ds(lax.rem(u, blocks) * p.block, p.block))
                dst = lambda u: self.raw(h, opposite, *at(u), c)
                self.add(4 * blocks, dst, dst, lambda u: self.cut(self.CB, half, h, *at(u)))
                copies[4 + h].start()
        elif s == 2:
            arrivals, copies = self.sum_arrivals(0, c), self.sum_copies(1, c)
            for kind in (2, 3, 4, 5):
                arrivals[kind].wait_recv()
            self.local(c)[2].wait()
            right, left, opposite = self.near(1, 1), self.near(1, 3), self.near(1, 2)
            blocks = p.units // p.block
            for i in (0, 1):
                srcs = self.kept(c, i, opposite, block)
                self.add(blocks, srcs[1], *srcs)
                copies[i].start()
            for way, i, b in ((0, 1, right), (1, 0, left)):
                self.add(blocks, lambda u: self.cut(self.SB, c, way, i, block(u)), *self.kept(c, i, b, block))
        elif s == 3:
            copies = self.sum_copies(1, c)
            for h, b in ((0, self.near(1, 1)), (1, self.near(1, 3))):
                copies[h].wait_recv()
                dst = lambda u: self.cut(self.SB, c, h, h, block(u))
                self.add(p.units // p.block, dst, *self.kept(c, h, b, block), dst)
                copies[2 + h].start()
            self.credit(1, c)
        elif s == 4:
            before, copies = self.sum_copies(1, c), self.sum_copies(2, c)
            for kind in (2, 3):
                before[kind].wait_recv()
            right, left, opposite = self.near(2, 1), self.near(2, 3), self.near(2, 2)
            for i in (0, 1):
                self.add(1, lambda u: self.cut(self.XC, c, i), *self.own_sum(c, i, opposite))
                copies[i].start()
            for way, i, z in ((0, 1, right), (1, 0, left)):
                self.add(1, lambda u: self.cut(self.SC, c, way, i), *self.own_sum(c, i, z))
        elif s == 5:
            copies = self.sum_copies(2, c)
            for h, z in ((0, self.near(2, 1)), (1, self.near(2, 3))):
                copies[h].wait_recv()
                dst = lambda u: self.cut(self.SC, c, h, h)
                self.add(1, dst, *self.own_sum(c, h, z), dst)
                copies[2 + h].start()
            if not p.down:
                self.credit(2, c)
        elif s == 6:
            before, copies = self.sum_copies(2, c), self.gather_copies(2, c)
            for kind in (2, 3):
                before[kind].wait_recv()

            @pl.when(c == 0)
            def _():
                for one in self.preload():
                    one.wait()
                if p.down:
                    self.moments(True)

            self.update(c)
            if not p.down:
                pl.semaphore_wait(self.free.at[c, 2], 2)
            copies[0].start()
            copies[1].start()
            for one in self.sent_from_out(c):
                one.wait_send()
            self.credit(0, c)
            if p.down:

                @pl.when(c == p.chunks - 1)
                def _():
                    self.moments(False)
        elif s in (7, 9, 11):
            phase = {7: 2, 9: 1, 11: 0}[s]
            arrivals, copies = self.gather_arrivals(phase, c), self.gather_copies(phase, c)
            arrivals[0].wait_recv()
            copies[2].start()
            arrivals[1].wait_recv()
            copies[3].start()
            if s == 11:
                self.sent(c)
        elif s in (8, 10):
            phase = {8: 1, 10: 0}[s]
            arrivals, copies = self.gather_arrivals(phase + 1, c), self.gather_copies(phase, c)
            arrivals[2].wait_recv()
            arrivals[3].wait_recv()
            if s == 8 and p.down:
                self.merge(c)
            pl.semaphore_wait(self.free.at[c, phase], 2)
            copies[0].start()
            copies[1].start()

    def sent_from_out(self, c):
        return [*self.sum_copies(0, c)[4:], *self.sum_copies(1, c)[:2]]

    def update(self, c):
        p = self.p
        cols = self.cols(c)
        z = self.me[2]
        for i in (0, 1):
            srcs = [*self.own_sum(c, i, z), *(lambda u, ref=ref: self.cut(ref, c, i) for ref in (self.LC, self.RC))]
            total = srcs[0](0)[...].astype(F32)
            for s in srcs[1:]:
                total = total + s(0)[...].astype(F32)
            g = total.astype(BF16).astype(F32).reshape(p.window * p.rows, self.width)
            mr, vr = (self.mb, self.vb) if p.down else (self.mout, self.vout)
            m = 0.9 * mr[i, :, cols] + 0.1 * g
            v = 0.95 * vr[i, :, cols] + 0.05 * g * g
            w = self.wb[i, :, :, cols].astype(F32).reshape(p.window * p.rows, self.width)
            w = (w - 0.02 * (m * lax.rsqrt(v + 1e-8) + 0.1 * w)).reshape(p.window, p.rows, self.width).astype(BF16)
            mr[i, :, cols] = m
            vr[i, :, cols] = v
            if p.down:
                self.cut(self.WN, c, z, i)[...] = w
            else:
                self.part(self.out, i, c, *self.me)[...] = w[0]

    def moments(self, into):
        first = 2 * self.at["z"]

        @pl.loop(0, 50)
        def _(r):
            for whole, held in ((self.mout, self.mb), (self.vout, self.vb)):
                for i in (0, 1):
                    if into:
                        held[i, pl.ds(first + r, 1), :] = whole[r, pl.ds(i, 1), :]
                    else:
                        whole[r, pl.ds(i, 1), :] = held[i, pl.ds(first + r, 1), :]

    def merge(self, c):
        p = self.p
        row = lax.broadcasted_iota(jnp.int32, (p.rows, self.width), 0)
        a, b = self.me[:2]
        for i in (0, 1):
            for z in range(4):
                low = 0 if z == 0 else 1
                high = 7 if z == 3 else 6
                self.raw(i, a, b, pl.ds(6 * z + low, high - low), c)[...] = self.cut(self.WN, c, z, i, pl.ds(low, high - low))[...]
                if z:
                    below = self.cut(self.WN, c, z - 1, i, 6)[...].astype(F32)
                    above = self.cut(self.WN, c, z, i, 0)[...].astype(F32)
                    self.raw(i, a, b, 6 * z, c)[...] = jnp.where(row < 2 * z, below, above).astype(BF16)

    def sent(self, c):
        waited = self.sum_copies(0, c)[:4] + self.sum_copies(1, c)[2:] + self.sum_copies(2, c)
        for copy in (*waited, *self.gather_copies(2, c), *self.gather_copies(1, c)):
            copy.wait_send()

    def finish(self, c):
        for copy in self.gather_copies(0, c):
            copy.wait_send()
        for arrival in self.gather_arrivals(0, c)[2:]:
            arrival.wait_recv()


def kernel(*refs):
    ins, outs, rest = refs[:12], refs[12:21], refs[21:]
    i = lax.axis_index("dp")
    at = {"x": lax.div(i, 16), "y": lax.rem(lax.div(i, 4), 4), "z": lax.rem(i, 4)}
    runs = []
    for n, p in enumerate(PARTS):
        buffers = dict(zip(SCRATCH, rest[n * len(SCRATCH) : (n + 1) * len(SCRATCH)]))
        runs.append(Run(p, at, *ins[n::3], *outs[n::3], **buffers))
    last = max(p.chunks for p in PARTS) + STAGES - 1

    barrier = pltpu.get_barrier_semaphore()
    for phase in range(3):
        for offset in (1, 3):
            pl.semaphore_signal(barrier, inc=1, device_id=runs[0].device(phase, offset), device_id_type=MESH)
    for run in runs:
        for one in run.preload():
            one.start()
    pl.semaphore_wait(barrier, 6)

    @pl.loop(0, last)
    def _(t):
        for s in range(STAGES):
            for run in runs:
                for group in run.p.groups:

                    @pl.when((t - s >= group[0]) & (t - s < group[1]))
                    def _(run=run, s=s, group=group):
                        run.use(group).stage(s, t - s)

    for run in runs:
        for group in run.p.groups:

            @pl.loop(group[0], group[1])
            def _(c, run=run, group=group):
                run.use(group).finish(c)


def sum_step_gather(terms, weights, m, v):
    shapes = [(2, 4, 4, 4, 16, 3200)] * 2 + [(2, 4, 4, 25, 8, 1024)]
    moments = [a.shape for a in m]
    args = [a.reshape(s) for group in (terms, weights) for a, s in zip(group, shapes, strict=True)] + [*m, *v]
    held = [one for p in PARTS for one in (lambda made: [made[name] for name in SCRATCH])(scratch(p))]
    hbm = pl.BlockSpec(memory_space=pl.ANY)
    vmem = pl.BlockSpec(memory_space=pltpu.VMEM)
    made = pl.pallas_call(
        kernel,
        name="sum_step_gather",
        out_shape=[pltpu.VMEM(s, BF16) for s in shapes] + [pltpu.VMEM(s, F32) for s in moments * 2],
        in_specs=[hbm] * 12,
        out_specs=[vmem] * 9,
        scratch_shapes=held,
        compiler_params=pltpu.CompilerParams(collective_id=0, has_side_effects=True, vmem_limit_bytes=VMEM_LIMIT),
    )(*args)
    return pl.pallas_call(
        write_out,
        name="write_out",
        out_shape=[jax.ShapeDtypeStruct(a.shape, a.dtype) for a in made],
        in_specs=[vmem] * 9,
        out_specs=[hbm] * 9,
        scratch_shapes=[pltpu.SemaphoreType.DMA((9, 2))],
        compiler_params=pltpu.CompilerParams(vmem_limit_bytes=VMEM_LIMIT),
    )(*(pltpu.with_memory_space_constraint(a, pltpu.VMEM) for a in made))


def write_out(*refs):
    ins, outs, sems = refs[:9], refs[9:18], refs[18]
    copies = []
    for n, (src, dst) in enumerate(zip(ins, outs, strict=True)):
        if n < 3:
            copies += [pltpu.make_async_copy(src.at[i], dst.at[i], sems.at[n, i]) for i in (0, 1)]
        else:
            copies.append(pltpu.make_async_copy(src, dst, sems.at[n, 0]))
    for one in copies:
        one.start()
    for one in copies:
        one.wait()


def solution(mesh):
    def step(*arrays):
        terms, weights, m, v = (arrays[i : i + 3] for i in (0, 3, 6, 9))
        turn = lambda a: [*a[:2], a[2].transpose(1, 0, 2)]
        out = sum_step_gather(terms, weights, turn(m), turn(v))
        new = [a.reshape(w.shape) for a, w in zip(out[:3], weights, strict=True)]
        return (*new, *turn(out[3:6]), *turn(out[6:9]))

    all_of, cut = P(None, None, None), P(None, "dp", None)
    return jax.shard_map(
        step,
        mesh=mesh,
        in_specs=(P(("rep", "dp"), None, None, None),) * 3 + (all_of,) * 3 + (cut,) * 6,
        out_specs=(P("rep", None, None),) * 3 + (P("rep", "dp", None),) * 6,
        check_vma=False,
    )
```
